16 devices in a mesh: data: 2 (over y, z), expert: 8 (over x, core).
Axes of the slice: x: 4, y: 2, z: 1, core: 2. Of those that a mesh axis runs over, the one named last changes fastest.
The devices are a block of a 4x4x8 slice.
Arguments:
- x_in: bfloat16 [65536, 768], P(('data', 'expert')), parts along dimension 0
- route_idx: int32 [65536, 4], P(('data', 'expert')), parts along dimension 0
- route_gate: float32 [65536, 4], P(('data', 'expert')), parts along dimension 0
- grad_y: bfloat16 [65536, 768], P(('data', 'expert')), parts along dimension 0
- w_in1: bfloat16 [16, 768, 1344], P('expert')
- w_in3: bfloat16 [16, 768, 1344], P('expert')
- w_out: bfloat16 [16, 1344, 768], P('expert')
Outputs:
- output 1: bfloat16 [65536, 768], P(('data', 'expert')), parts along dimension 0
- output 2: bfloat16 [65536, 768], P(('data', 'expert')), parts along dimension 0
- output 3: float32 [32, 768, 1344], P(('data', 'expert')), parts along dimension 0
- output 4: float32 [32, 768, 1344], P(('data', 'expert')), parts along dimension 0
- output 5: float32 [32, 1344, 768], P(('data', 'expert')), parts along dimension 0
- output 6: float32 [4, 768, 1344], P('data', None, 'expert'), parts along dimension 0
- output 7: float32 [4, 768, 1344], P('data', None, 'expert'), parts along dimension 0
- output 8: float32 [4, 1344, 768], P('data', 'expert'), parts along dimension 0
There are 2 independent parts. The reference program is written for one: setup_inputs(seed, part) draws one part's arguments, and reference() takes and returns one part's arrays. A program takes and returns all parts, laid end to end along the dimension named above; an argument that names none is the same for every part.
All inputs are finite; a program needn't handle non-finite values.
Results may differ from the reference program's by a relative error of at most 0.0112156.
Values are sent between devices in bfloat16 or wider.
A program may use at most 768 MiB of HBM per device.

```python
import jax
import jax.numpy as jnp
from jax import lax

WIDTH = 768
FFN_WIDTH = 1344
EXPERTS = 16
TOP_K = 4
HOT_EXPERTS = 2
TOKENS = 4096
GROUP_SIZE = 8
CAPACITY = 1056


def draw_routing(key):
    tok_count = GROUP_SIZE * TOKENS
    stride = EXPERTS // HOT_EXPERTS
    cold_count = EXPERTS - HOT_EXPERTS
    sub_keys = jax.random.split(key, 5)
    coin_flip = jax.random.randint(sub_keys[0], (tok_count,), 0, 2)
    draw_one = jax.random.randint(sub_keys[1], (tok_count,), 0, cold_count)
    draw_two = jax.random.randint(sub_keys[2], (tok_count,), 0, cold_count)
    is_forced = (jnp.arange(tok_count) % TOKENS) < CAPACITY
    base_pos = jnp.where(coin_flip == 0, jnp.minimum(draw_one, draw_two), draw_one)
    base_pos = jnp.where(is_forced, 0, base_pos)
    slot_ids = jnp.arange(TOP_K)[None, :]
    cold_pos = (base_pos[:, None] + slot_ids) % cold_count
    cold_ids = (cold_pos // (stride - 1)) * stride + 1 + cold_pos % (stride - 1)
    hot_roll = jax.random.randint(sub_keys[3], (tok_count, 1), 0, HOT_EXPERTS)
    hot_ids = ((slot_ids + hot_roll) % HOT_EXPERTS) * stride
    hot_pick = jax.random.randint(sub_keys[4], (tok_count, TOP_K), 0, 4) < 3
    hot_pick = hot_pick & (slot_ids < HOT_EXPERTS) & jnp.logical_not(is_forced[:, None] & (slot_ids == 0))
    return jnp.where(hot_pick, hot_ids, cold_ids).astype(jnp.int32)


def setup_inputs(seed: int = 0, part: int = 0) -> dict:
    part_key = jax.random.fold_in(jax.random.key(seed), part)
    sub_keys = jax.random.split(part_key, 4)
    w_keys = jax.random.split(jax.random.key(seed + 1), 3)
    tok_count = GROUP_SIZE * TOKENS
    x_in = jax.random.normal(sub_keys[0], (tok_count, WIDTH), jnp.float32).astype(jnp.bfloat16)
    route_idx = draw_routing(sub_keys[1])
    route_gate = jax.random.uniform(sub_keys[2], (tok_count, TOP_K), jnp.float32, 0.2, 1.0)
    grad_y = jax.random.normal(sub_keys[3], (tok_count, WIDTH), jnp.float32).astype(jnp.bfloat16)
    w_in1 = (jax.random.normal(w_keys[0], (EXPERTS, WIDTH, FFN_WIDTH), jnp.float32) * WIDTH ** -0.5).astype(jnp.bfloat16)
    w_in3 = (jax.random.normal(w_keys[1], (EXPERTS, WIDTH, FFN_WIDTH), jnp.float32) * WIDTH ** -0.5).astype(jnp.bfloat16)
    w_out = (jax.random.normal(w_keys[2], (EXPERTS, FFN_WIDTH, WIDTH), jnp.float32) * FFN_WIDTH ** -0.5).astype(jnp.bfloat16)
    return {"x_in": x_in, "route_idx": route_idx, "route_gate": route_gate, "grad_y": grad_y, "w_in1": w_in1, "w_in3": w_in3, "w_out": w_out}


def route_plan(idx_dev, gate_dev):
    slot_hits = idx_dev[:, :, None] == jnp.arange(EXPERTS, dtype=jnp.int32)[None, None, :]
    counts = jnp.sum(slot_hits.astype(jnp.int32), axis=1)
    before = jnp.cumsum(counts, axis=0) - counts
    slot_rank = jnp.sum(jnp.where(slot_hits, before[:, None, :], 0), axis=2)
    kept_mask = (idx_dev % (EXPERTS // HOT_EXPERTS) != 0) & (slot_rank < CAPACITY)
    dest_pos = jnp.where(kept_mask, idx_dev * CAPACITY + slot_rank, EXPERTS * CAPACITY)
    flat_dest = dest_pos.reshape(-1)
    tok_of_slot = jnp.arange(TOKENS * TOP_K, dtype=jnp.int32) // TOP_K
    slot_tok = jnp.full((EXPERTS * CAPACITY + 1,), TOKENS, jnp.int32).at[flat_dest].set(tok_of_slot)[:-1]
    slot_gate = jnp.zeros((EXPERTS * CAPACITY + 1,), jnp.float32).at[flat_dest].set(gate_dev.reshape(-1))[:-1]
    return dest_pos, slot_tok, slot_gate


def expert_pass(x_rows, do_rows, weight_a, weight_b, weight_c):
    pre_a = jnp.dot(x_rows, weight_a, preferred_element_type=jnp.float32).astype(jnp.bfloat16)
    pre_b = jnp.dot(x_rows, weight_b, preferred_element_type=jnp.float32).astype(jnp.bfloat16)
    act_a = pre_a.astype(jnp.float32)
    sig_a = jax.nn.sigmoid(act_a)
    hidden = (act_a * sig_a * pre_b.astype(jnp.float32)).astype(jnp.bfloat16)
    out_rows = jnp.dot(hidden, weight_c, preferred_element_type=jnp.float32).astype(jnp.bfloat16)
    d_hidden = jnp.dot(do_rows, weight_c.T, preferred_element_type=jnp.float32).astype(jnp.bfloat16).astype(jnp.float32)
    d_pre_a = (d_hidden * pre_b.astype(jnp.float32) * sig_a * (1.0 + act_a * (1.0 - sig_a))).astype(jnp.bfloat16)
    d_pre_b = (d_hidden * act_a * sig_a).astype(jnp.bfloat16)
    dx_rows = (jnp.dot(d_pre_a, weight_a.T, preferred_element_type=jnp.float32) + jnp.dot(d_pre_b, weight_b.T, preferred_element_type=jnp.float32)).astype(jnp.bfloat16)
    grad_a = jnp.dot(x_rows.T, d_pre_a, preferred_element_type=jnp.float32)
    grad_b = jnp.dot(x_rows.T, d_pre_b, preferred_element_type=jnp.float32)
    grad_c = jnp.dot(hidden.T, do_rows, preferred_element_type=jnp.float32)
    return out_rows, dx_rows, grad_a, grad_b, grad_c


def reference(x_in, route_idx, route_gate, grad_y, w_in1, w_in3, w_out):
    stride = EXPERTS // HOT_EXPERTS
    hot_ids = jnp.arange(HOT_EXPERTS, dtype=jnp.int32) * stride
    hot_gate = jnp.sum(jnp.where(route_idx[:, :, None] == hot_ids[None, None, :], route_gate[:, :, None], 0.0), axis=1)

    def hot_one(h_pos):
        expert_id = h_pos * stride
        do_rows = (grad_y.astype(jnp.float32) * hot_gate[:, h_pos][:, None]).astype(jnp.bfloat16)
        return expert_pass(x_in, do_rows, w_in1[expert_id], w_in3[expert_id], w_out[expert_id])

    hot_out, hot_dx, hot_ga, hot_gb, hot_gc = lax.map(hot_one, jnp.arange(HOT_EXPERTS))
    y_hot = jnp.sum(hot_gate.T[:, :, None] * hot_out.astype(jnp.float32), axis=0)
    dx_hot = jnp.sum(hot_dx.astype(jnp.float32), axis=0)

    def plan_dev(dev_args):
        idx_dev, gate_dev, x_dev, gy_dev = dev_args
        dest_pos, slot_tok, slot_gate = route_plan(idx_dev, gate_dev)
        x_buf = jnp.take(x_dev, slot_tok, axis=0, mode="fill", fill_value=0)
        do_buf = (jnp.take(gy_dev, slot_tok, axis=0, mode="fill", fill_value=0).astype(jnp.float32) * slot_gate[:, None]).astype(jnp.bfloat16)
        return dest_pos, x_buf, do_buf

    idx_devs = route_idx.reshape(GROUP_SIZE, TOKENS, TOP_K)
    gate_devs = route_gate.reshape(GROUP_SIZE, TOKENS, TOP_K)
    dest_all, x_bufs, do_bufs = lax.map(plan_dev, (idx_devs, gate_devs, x_in.reshape(GROUP_SIZE, TOKENS, WIDTH), grad_y.reshape(GROUP_SIZE, TOKENS, WIDTH)))
    row_count = GROUP_SIZE * CAPACITY
    x_rows = x_bufs.reshape(GROUP_SIZE, EXPERTS, CAPACITY, WIDTH).transpose(1, 0, 2, 3).reshape(EXPERTS, row_count, WIDTH)
    do_rows = do_bufs.reshape(GROUP_SIZE, EXPERTS, CAPACITY, WIDTH).transpose(1, 0, 2, 3).reshape(EXPERTS, row_count, WIDTH)

    def cold_one(ex_args):
        return expert_pass(ex_args[0], ex_args[1], ex_args[2], ex_args[3], ex_args[4])

    cold_out, cold_dx, grad_w1, grad_w3, grad_w2 = lax.map(cold_one, (x_rows, do_rows, w_in1, w_in3, w_out))
    out_devs = cold_out.reshape(EXPERTS, GROUP_SIZE, CAPACITY, WIDTH).transpose(1, 0, 2, 3).reshape(GROUP_SIZE, EXPERTS * CAPACITY, WIDTH)
    dx_devs = cold_dx.reshape(EXPERTS, GROUP_SIZE, CAPACITY, WIDTH).transpose(1, 0, 2, 3).reshape(GROUP_SIZE, EXPERTS * CAPACITY, WIDTH)

    def collect_dev(dev_args):
        dest_pos, gate_dev, out_buf, dx_buf = dev_args
        out_slots = jnp.take(out_buf, dest_pos, axis=0, mode="fill", fill_value=0).astype(jnp.float32)
        dx_slots = jnp.take(dx_buf, dest_pos, axis=0, mode="fill", fill_value=0).astype(jnp.float32)
        return jnp.sum(gate_dev[:, :, None] * out_slots, axis=1), jnp.sum(dx_slots, axis=1)

    y_cold, dx_cold = lax.map(collect_dev, (dest_all, gate_devs, out_devs, dx_devs))
    y_out = (y_hot + y_cold.reshape(-1, WIDTH)).astype(jnp.bfloat16)
    grad_x = (dx_hot + dx_cold.reshape(-1, WIDTH)).astype(jnp.bfloat16)
    return (y_out, grad_x, grad_w1, grad_w3, grad_w2, hot_ga, hot_gb, hot_gc)
```

```python
import functools

import jax
import jax.numpy as jnp
from jax import lax
from jax.experimental import pallas as pl
from jax.experimental.pallas import tpu as pltpu
from jax.sharding import PartitionSpec as P


HOT_COUNT = 2
F32 = jnp.float32
BF16 = jnp.bfloat16
VMEM_BYTES = 64_000_000
RADIX = 32


def capacity_of(tok_count, top_k, n_exp):
    return 8 * ((9 * top_k * tok_count) // (80 * (n_exp - HOT_COUNT)) + 1)


def tile_of(slot_cap, most):
    return max(t for t in range(16, most + 1, 16) if slot_cap % t == 0)


def running_count(hits):
    rows, toks = hits.shape
    lane = 128
    blocks = toks // lane
    tri = (jnp.arange(lane)[:, None] <= jnp.arange(lane)[None, :]).astype(BF16)
    inner = jnp.einsum("rbl,lm->rbm", hits.astype(BF16).reshape(rows, blocks, lane), tri, preferred_element_type=F32)
    tot = inner[:, :, -1]
    strict = jnp.arange(blocks)[:, None] < jnp.arange(blocks)[None, :]
    outer = jnp.sum(jnp.where(strict[None], tot[:, :, None], 0.0), axis=1)
    return (inner + outer[:, :, None]).reshape(rows, toks).astype(jnp.int32)


def slot_lists(hits, gates, slot_cap):
    rows, toks = hits.shape
    rank = running_count(hits) - 1
    kept = hits & (rank < slot_cap)
    n_q = -(-slot_cap // RADIX)
    q_hot = ((rank // RADIX)[:, :, None] == jnp.arange(n_q)[None, None, :]) & kept[:, :, None]
    r_hot = (rank % RADIX)[:, :, None] == jnp.arange(RADIX)[None, None, :]
    tok = jnp.broadcast_to(jnp.arange(toks, dtype=jnp.int32)[None], (rows, toks))
    top = jnp.finfo(BF16).max.astype(F32)
    g_hi = jnp.minimum(lax.reduce_precision(gates, 8, 7), top)
    g_mid = lax.reduce_precision(gates - g_hi, 8, 7)
    g_lo = gates - g_hi - g_mid
    vals = jnp.stack([(tok // 64).astype(F32), (tok % 64).astype(F32), g_hi, g_mid, g_lo], axis=1).astype(BF16)
    picks = jnp.where(r_hot[:, None], vals[:, :, :, None], 0).astype(BF16)
    res = jnp.einsum("etq,evtr->evqr", q_hot.astype(BF16), picks, preferred_element_type=F32)
    res = res.reshape(rows, 5, n_q * RADIX)[:, :, :slot_cap]
    slot_tok = (res[:, 0] * 64 + res[:, 1]).astype(jnp.int32)
    slot_gate = (res[:, 2] + res[:, 3]) + res[:, 4]
    counts = jnp.sum(kept.astype(jnp.int32), axis=1)
    pos = jnp.arange(slot_cap, dtype=jnp.int32)[None]
    return jnp.where(pos < counts[:, None], slot_tok, pos % toks), slot_gate, counts


def dot_nn(lhs, rhs):
    return lax.dot_general(lhs, rhs, (((1,), (0,)), ((), ())), preferred_element_type=F32)


def dot_nt(lhs, rhs):
    return lax.dot_general(lhs, rhs, (((1,), (1,)), ((), ())), preferred_element_type=F32)


def dot_tn(lhs, rhs):
    return lax.dot_general(lhs, rhs, (((0,), (0,)), ((), ())), preferred_element_type=F32)


def tile_grads(x_rows, u_rows, w1, w3, w2):
    pre_a = dot_nt(x_rows, w1).astype(BF16).astype(F32)
    pre_b = dot_nt(x_rows, w3).astype(BF16).astype(F32)
    d_hid = dot_nt(u_rows, w2).astype(BF16).astype(F32)
    sig = jax.nn.sigmoid(pre_a)
    silu = pre_a * sig
    hid = (silu * pre_b).astype(BF16)
    d_a = (d_hid * pre_b * sig * (1.0 + pre_a * (1.0 - sig))).astype(BF16)
    d_b = (d_hid * silu).astype(BF16)
    return hid, d_a, d_b


def local_kernel(n_tiles, rows, cap, tok_ref, cnt_ref, dev_ref, lst_ref, x_ref, gy_ref, gate_ref, w1_ref, w3_ref, w2_ref, y0_ref, dx0_ref,
                 y_ref, dx_ref, y_acc, dx_acc, o_buf, d_buf, sems):
    e = pl.program_id(0)
    k = pl.program_id(1)
    toks = y0_ref.shape[0]

    @pl.when((e == 0) & (k == 0))
    def _():
        c0 = pltpu.make_async_copy(y0_ref, y_acc.at[pl.ds(0, toks)], sems.at[0])
        c1 = pltpu.make_async_copy(dx0_ref, dx_acc.at[pl.ds(0, toks)], sems.at[1])
        c0.start()
        c1.start()
        c0.wait()
        c1.wait()

    left = cnt_ref[lst_ref[e]] - k * rows

    @pl.when(left > 0)
    def _():
        live = lax.broadcasted_iota(jnp.int32, (rows, 1), 0) < left
        x_rows = jnp.where(live, x_ref[...].astype(F32), 0.0).astype(BF16)
        gate = gate_ref[...]
        u_rows = jnp.where(live, gy_ref[...].astype(F32) * gate, 0.0).astype(BF16)
        hid, d_a, d_b = tile_grads(x_rows, u_rows, w1_ref[0], w3_ref[0], w2_ref[0])
        o_buf[...] = dot_nn(hid, w2_ref[0]).astype(BF16).astype(F32) * gate
        d_buf[...] = (dot_nn(d_a, w1_ref[0]) + dot_nn(d_b, w3_ref[0])).astype(BF16).astype(F32)
        base = lst_ref[e] * cap + k * rows
        step = 8

        @pl.loop(0, pl.cdiv(jnp.minimum(left, rows), step))
        def _(i):
            r0 = pl.multiple_of(i * step, step)
            o_blk = o_buf[pl.ds(r0, step), :]
            d_blk = d_buf[pl.ds(r0, step), :]
            dst = [jnp.where(r0 + j < left, tok_ref[base + r0 + j], toks) for j in range(step)]
            old_y = [y_acc[pl.ds(dst[j], 1), :] for j in range(step)]
            old_d = [dx_acc[pl.ds(dst[j], 1), :] for j in range(step)]
            for j in range(step):
                y_acc[pl.ds(dst[j], 1), :] = old_y[j] + o_blk[j:j + 1]
                dx_acc[pl.ds(dst[j], 1), :] = old_d[j] + d_blk[j:j + 1]

    @pl.when((e == pl.num_programs(0) - 1) & (k == n_tiles - 1))
    def _():
        if y_ref.dtype == F32:
            c0 = pltpu.make_async_copy(y_acc.at[pl.ds(0, toks)], y_ref, sems.at[0])
            c1 = pltpu.make_async_copy(dx_acc.at[pl.ds(0, toks)], dx_ref, sems.at[1])
            c0.start()
            c1.start()
            c0.wait()
            c1.wait()
        else:
            y_ref[...] = y_acc[pl.ds(0, toks), :].astype(BF16)
            dx_ref[...] = dx_acc[pl.ds(0, toks), :].astype(BF16)


def local_experts(pair_rows, slot_tok, slot_gate, counts, dev, lst, w1, w3, w2, y0, dx0, out_dtype):
    n_exp, cap = dev.shape[0], slot_tok.shape[1]
    width = y0.shape[1]
    ffn = w1.shape[1]
    toks = y0.shape[0]
    rows = tile_of(cap, 352)
    n_tiles = cap // rows

    def row_map(col, e, k, tok, cnt, dev, lst):
        last = jnp.maximum(pl.cdiv(cnt[lst[e]], rows) - 1, 0)
        return (lst[e] * n_tiles + jnp.minimum(k, last), col)

    x_spec, gy_spec = (pl.BlockSpec((rows, width), functools.partial(row_map, col)) for col in range(2))
    w_spec = pl.BlockSpec((1, ffn, width), lambda e, k, tok, cnt, dev, lst: (dev[e], 0, 0))
    any_spec = pl.BlockSpec(memory_space=pl.ANY)
    if out_dtype == F32:
        out_spec = any_spec
    else:
        out_spec = pl.BlockSpec((toks, width), lambda e, k, tok, cnt, dev, lst: (0, 0), pipeline_mode=pl.Buffered(1))
    grid_spec = pltpu.PrefetchScalarGridSpec(
        num_scalar_prefetch=4, grid=(n_exp, n_tiles),
        in_specs=[x_spec, gy_spec, pl.BlockSpec((rows, 1), functools.partial(row_map, 0)), w_spec, w_spec, w_spec, any_spec, any_spec],
        out_specs=[out_spec, out_spec],
        scratch_shapes=[pltpu.VMEM((toks + 8, width), F32), pltpu.VMEM((toks + 8, width), F32),
                        pltpu.VMEM((rows, width), F32), pltpu.VMEM((rows, width), F32), pltpu.SemaphoreType.DMA((2,))])
    return pl.pallas_call(
        functools.partial(local_kernel, n_tiles, rows, cap), grid_spec=grid_spec,
        out_shape=[jax.ShapeDtypeStruct((toks, width), out_dtype)] * 2,
        cost_estimate=pl.CostEstimate(flops=12 * n_exp * cap * width * ffn, bytes_accessed=8 * toks * width, transcendentals=0),
        compiler_params=pltpu.CompilerParams(dimension_semantics=("arbitrary", "arbitrary"), vmem_limit_bytes=VMEM_BYTES),
    )(slot_tok.reshape(-1), counts, dev, lst, pair_rows, pair_rows, slot_gate.reshape(-1, 1), w1, w3, w2, y0, dx0)


def owner_kernel(n_tiles, rows, cnt_ref, x_ref, gy_ref, gate_ref, w1_ref, w3_ref, w2_ref, g1_ref, g3_ref, g2_ref):
    e = pl.program_id(0)
    k = pl.program_id(1)

    @pl.when(k == 0)
    def _():
        g1_ref[...] = jnp.zeros_like(g1_ref)
        g3_ref[...] = jnp.zeros_like(g3_ref)
        g2_ref[...] = jnp.zeros_like(g2_ref)

    left = cnt_ref[k // n_tiles * pl.num_programs(0) + e] - (k % n_tiles) * rows

    @pl.when(left > 0)
    def _():
        live = lax.broadcasted_iota(jnp.int32, (rows, 1), 0) < left
        x_rows = jnp.where(live, x_ref[...].astype(F32), 0.0).astype(BF16)
        u_rows = jnp.where(live, gy_ref[...].astype(F32) * gate_ref[...], 0.0).astype(BF16)
        hid, d_a, d_b = tile_grads(x_rows, u_rows, w1_ref[0], w3_ref[0], w2_ref[0])
        g1_ref[0] += dot_tn(d_a, x_rows)
        g3_ref[0] += dot_tn(d_b, x_rows)
        g2_ref[0] += dot_tn(hid, u_rows)


def owner_grads(pair_rows, slot_gate, counts, w1, w3, w2):
    n_exp, ffn, width = w1.shape
    lists, cap = slot_gate.shape
    rows = tile_of(cap, 528)
    n_tiles = cap // rows
    per_exp = lists // n_exp

    def row_map(col, e, k, cnt):
        src = k // n_tiles * n_exp + e
        last = jnp.maximum(pl.cdiv(cnt[src], rows) - 1, 0)
        return (src * n_tiles + jnp.minimum(k % n_tiles, last), col)

    x_spec, gy_spec = (pl.BlockSpec((rows, width), functools.partial(row_map, col)) for col in range(2))
    w_spec = pl.BlockSpec((1, ffn, width), lambda e, k, cnt: (e, 0, 0))
    grid_spec = pltpu.PrefetchScalarGridSpec(
        num_scalar_prefetch=1, grid=(n_exp, per_exp * n_tiles),
        in_specs=[x_spec, gy_spec, pl.BlockSpec((rows, 1), functools.partial(row_map, 0)), w_spec, w_spec, w_spec],
        out_specs=[w_spec, w_spec, w_spec])
    return pl.pallas_call(
        functools.partial(owner_kernel, n_tiles, rows), grid_spec=grid_spec,
        out_shape=[jax.ShapeDtypeStruct((n_exp, ffn, width), F32)] * 3,
        cost_estimate=pl.CostEstimate(flops=12 * lists * cap * width * ffn, bytes_accessed=4 * lists * cap * width, transcendentals=0),
        compiler_params=pltpu.CompilerParams(dimension_semantics=("arbitrary", "arbitrary"), vmem_limit_bytes=VMEM_BYTES),
    )(counts, pair_rows, pair_rows, slot_gate.reshape(-1, 1), w1, w3, w2)


def hot_kernel(x_ref, gy_ref, gate_ref, w1_ref, w3_ref, w2_ref, y_in, dx_in, y_ref, dx_ref, g1_ref, g3_ref, g2_ref):
    @pl.when(pl.program_id(0) == 0)
    def _():
        g1_ref[...] = jnp.zeros_like(g1_ref)
        g3_ref[...] = jnp.zeros_like(g3_ref)
        g2_ref[...] = jnp.zeros_like(g2_ref)

    x_rows = x_ref[...]
    gate = gate_ref[...]
    u_rows = (gy_ref[...].astype(F32) * gate).astype(BF16)
    hid, d_a, d_b = tile_grads(x_rows, u_rows, w1_ref[...], w3_ref[...], w2_ref[...])
    y_new = dot_nn(hid, w2_ref[...]).astype(BF16).astype(F32) * gate
    dx_new = (dot_nn(d_a, w1_ref[...]) + dot_nn(d_b, w3_ref[...])).astype(BF16).astype(F32)
    y_ref[...] = y_new if y_in is None else y_in[...] + y_new
    dx_ref[...] = dx_new if dx_in is None else dx_in[...] + dx_new
    g1_ref[...] += dot_tn(d_a, x_rows)
    g3_ref[...] += dot_tn(d_b, x_rows)
    g2_ref[...] += dot_tn(hid, u_rows)


def hot_expert(x_in, grad_y, gate, w1, w3, w2, y0, dx0):
    toks, width = x_in.shape
    ffn = w1.shape[0]
    rows = 512
    while toks % rows:
        rows //= 2
    row_spec = pl.BlockSpec((rows, width), lambda k: (k, 0))
    keep = dict(pipeline_mode=pl.Buffered(1))
    w_spec = pl.BlockSpec((ffn, width), lambda k: (0, 0), **keep)
    in_specs = [row_spec, row_spec, pl.BlockSpec((rows, 1), lambda k: (k, 0)), w_spec, w_spec, w_spec]
    args = [x_in, grad_y, gate, w1, w3, w2]
    if y0 is None:
        def body(*refs):
            hot_kernel(*refs[:6], None, None, *refs[6:])
    else:
        body = hot_kernel
        in_specs += [row_spec, row_spec]
        args += [y0, dx0]
    return pl.pallas_call(
        body, grid=(toks // rows,), in_specs=in_specs,
        out_specs=[row_spec, row_spec, w_spec, w_spec, w_spec],
        out_shape=[jax.ShapeDtypeStruct((toks, width), F32)] * 2 + [jax.ShapeDtypeStruct((ffn, width), F32)] * 3,
        cost_estimate=pl.CostEstimate(flops=18 * toks * width * ffn, bytes_accessed=16 * toks * width, transcendentals=0),
        compiler_params=pltpu.CompilerParams(dimension_semantics=("arbitrary",), vmem_limit_bytes=VMEM_BYTES),
    )(*args)


def solution(mesh):
    group_n = mesh.shape["expert"]
    tok_spec = P(("data", "expert"))
    w_spec = P("expert")
    hot_spec_in = P("data", None, "expert")
    hot_spec_out = P("data", "expert", None)

    def local_step(x_in, route_idx, route_gate, grad_y, w_in1, w_in3, w_out):
        tok_count = x_in.shape[0]
        top_k = route_idx.shape[1]
        local_n = w_in1.shape[0]
        n_exp = local_n * group_n
        slot_cap = capacity_of(tok_count, top_k, n_exp)
        stride = n_exp // HOT_COUNT
        weights = (jnp.swapaxes(w_in1, 1, 2), jnp.swapaxes(w_in3, 1, 2), w_out)
        ffn, width = weights[2].shape[1:]

        def gather(v):
            return lax.all_gather(v, "expert", axis=0, tiled=True)

        def scatter_sum(v):
            return lax.psum_scatter(v, "expert", scatter_dimension=0, tiled=True)

        w_all = []
        for j in range(local_n):
            w_all.append([gather(w[j]).reshape(group_n, ffn, width) for w in weights])

        idx_t = route_idx.T
        gate_t = route_gate.T
        experts = jnp.arange(n_exp, dtype=jnp.int32)
        match = (idx_t[None] == experts[:, None, None]) & (experts % stride != 0)[:, None, None]
        slot_tok, slot_gate, counts = slot_lists(jnp.any(match, axis=1), jnp.sum(jnp.where(match, gate_t[None], 0.0), axis=1), slot_cap)
        pair = jnp.take(jnp.concatenate([x_in, grad_y], axis=1), slot_tok.reshape(-1), axis=0, mode="clip")

        def exchange(v):
            return lax.all_to_all(v, "expert", 0, 0, tiled=True)

        own_pair = exchange(pair.reshape(group_n, local_n, slot_cap, 2 * width)).reshape(-1, 2 * width)
        own_gate = exchange(slot_gate.reshape(group_n, local_n, slot_cap)).reshape(-1, slot_cap)
        own_cnt = exchange(counts.reshape(group_n, local_n)).reshape(-1)

        hot_ids = jnp.arange(HOT_COUNT, dtype=jnp.int32) * stride
        hot_gate = jnp.sum(jnp.where(idx_t[None] == hot_ids[:, None, None], gate_t[None], 0.0), axis=1)
        hot_gate, pair, own_gate, own_cnt = lax.optimization_barrier((hot_gate, pair, own_gate, own_cnt))

        y_sum, dx_sum, hot_g = None, None, []
        for i in range(HOT_COUNT):
            j, d = (i * stride) % local_n, (i * stride) // local_n
            y_sum, dx_sum, *grads = hot_expert(x_in, grad_y, hot_gate[i][:, None], *[w[d] for w in w_all[j]], y_sum, dx_sum)
            hot_g.append([scatter_sum(g) for g in grads])

        for j in range(local_n):
            part = [d for d in range(group_n) if (d * local_n + j) % stride != 0]
            dev = jnp.asarray(part, jnp.int32)
            y_sum, dx_sum = local_experts(pair, slot_tok, slot_gate, counts, dev, dev * local_n + j, *w_all[j], y_sum, dx_sum,
                                          BF16 if j == local_n - 1 else F32)

        grad_w1, grad_w3, grad_w2 = owner_grads(own_pair, own_gate, own_cnt, *weights)
        hot_g, grad_w2 = lax.optimization_barrier((hot_g, grad_w2))
        hot_g1 = jnp.stack([g[0].T for g in hot_g])
        hot_g3 = jnp.stack([g[1].T for g in hot_g])
        hot_g2 = jnp.stack([g[2] for g in hot_g])
        return y_sum, dx_sum, jnp.swapaxes(grad_w1, 1, 2), jnp.swapaxes(grad_w3, 1, 2), grad_w2, hot_g1, hot_g3, hot_g2

    return jax.shard_map(local_step, mesh=mesh,
                         in_specs=(tok_spec, tok_spec, tok_spec, tok_spec, w_spec, w_spec, w_spec),
                         out_specs=(tok_spec, tok_spec, tok_spec, tok_spec, tok_spec, hot_spec_in, hot_spec_in, hot_spec_out),
                         check_vma=False)
```
